8 devices in a mesh: dp: 2 (over y, z), sp: 4 (over x, core).
Axes of the slice: x: 2, y: 2, z: 1, core: 2. Of those that a mesh axis runs over, the one named last changes fastest.
Arguments:
- x: bfloat16 [4096, 5120], P(('dp', 'sp')), parts along dimension 0
- gain: bfloat16 [5120], replicated
- wq: bfloat16 [5120, 5120], replicated
- wk: bfloat16 [5120, 5120], replicated
- wv: bfloat16 [5120, 5120], replicated
- wo: bfloat16 [5120, 5120], replicated
Outputs:
- output: bfloat16 [4096, 5120], P(('dp', 'sp')), parts along dimension 0
There are 2 independent parts. The reference program is written for one: setup_inputs(seed, part) draws one part's arguments, and reference() takes and returns one part's arrays. A program takes and returns all parts, laid end to end along the dimension named above; an argument that names none is the same for every part.
All inputs are finite; a program needn't handle non-finite values.
Results may differ from the reference program's by a relative error of at most 0.012.
Values are sent between devices in bfloat16 or wider.
A program may use at most 2 GiB of HBM per device.

```python
import jax
import jax.numpy as jnp
from jax import lax

ROWS = 2048
D = 5120
HEADS = 40
KV_HEADS = 40
HEAD = 128
THETA = 10000


def setup_inputs(seed: int = 0, part: int = 0) -> dict:
    kx, kn, kq, kk, kv, ko = jax.random.split(jax.random.key(seed), 6)

    def weights(key, rows, columns):
        return jax.random.normal(key, (rows, columns), jnp.float32) * rows**-0.5

    drawn = {
        "x": jax.random.normal(jax.random.fold_in(kx, part), (ROWS, D), jnp.float32),
        "gain": 1 + 0.1 * jax.random.normal(kn, (D,), jnp.float32),
        "wq": 2 * weights(kq, D, HEADS * HEAD),
        "wk": 2 * weights(kk, D, KV_HEADS * HEAD),
        "wv": 4 * weights(kv, D, KV_HEADS * HEAD),
        "wo": weights(ko, HEADS * HEAD, D),
    }
    return {k: v.astype(jnp.bfloat16) for k, v in drawn.items()}


def normed(x, gain):
    wide = x.astype(jnp.float32)
    scale = lax.rsqrt(jnp.mean(wide * wide, -1, keepdims=True) + 1e-6)
    return (wide * scale * gain.astype(jnp.float32)).astype(jnp.bfloat16)


def turned(t, place, theta):
    half = t.shape[-1] // 2
    angle = place.astype(jnp.float32)[:, None] * theta ** (-jnp.arange(half, dtype=jnp.float32) / half)
    cos, sin = jnp.cos(angle)[:, None], jnp.sin(angle)[:, None]
    a, b = t[..., :half].astype(jnp.float32), t[..., half:].astype(jnp.float32)
    return jnp.concatenate([a * cos - b * sin, b * cos + a * sin], -1).astype(jnp.bfloat16)


def matmul(a, w):
    return jnp.dot(a, w, preferred_element_type=jnp.float32).astype(jnp.bfloat16)


def einsum(form, a, b):
    return jnp.einsum(form, a.astype(jnp.float32), b.astype(jnp.float32))


def attention(q, k, v):
    scores = einsum("tgsd,ugd->gstu", q, k) * q.shape[-1] ** -0.5
    token = jnp.arange(q.shape[0])
    scores = jnp.where(token[:, None] >= token, scores, -jnp.inf)
    weights = jax.nn.softmax(scores, -1).astype(jnp.bfloat16)
    return einsum("gstu,ugd->tgsd", weights, v).astype(jnp.bfloat16)


def reference(x, gain, wq, wk, wv, wo):
    a, place = normed(x, gain), jnp.arange(ROWS)
    q = turned(matmul(a, wq).reshape(ROWS, HEADS, HEAD), place, THETA).reshape(ROWS, KV_HEADS, -1, HEAD)
    k = turned(matmul(a, wk).reshape(ROWS, KV_HEADS, HEAD), place, THETA)
    v = matmul(a, wv).reshape(ROWS, KV_HEADS, HEAD)
    seen = attention(q, k, v).reshape(ROWS, HEADS * HEAD)
    return (x.astype(jnp.float32) + jnp.dot(seen, wo, preferred_element_type=jnp.float32)).astype(jnp.bfloat16)
```

```python
import functools

import jax
import jax.numpy as jnp
from jax import lax
from jax.experimental import pallas as pl
from jax.experimental.pallas import tpu as pltpu
from jax.sharding import PartitionSpec as P

HEAD = 128
THETA = 10000
NEG = -1e30
HIDDEN = 2 * NEG
LOG2E = 1.4426950408889634
TILE = 256
STRIP = 256


def _dot(a, b):
    return jnp.dot(a, b, preferred_element_type=jnp.float32)


def _kernel(x_ref, gain_ref, cos_t, sin_t, cos_f, sin_f, wq_ref, wk_ref, wv_ref, wo_ref, y_ref,
            a_s, w_s, qt_s, k_s, vt_s, xb_s, lx_s, o_s, xin_s, yout_s,
            bar_x, w_sem, ax_send, ax_recv, q_send, q_recv, o_send, o_recv, l_send, l_recv, t_send, t_recv, xin_sem, yout_sem):
    own, depth = x_ref.shape
    pairs = k_s.shape[0] // 2
    wide = pairs * TILE
    n_out = depth // TILE
    e = HEAD**-0.5 * LOG2E
    me = lax.axis_index("sp")
    chip, core = me // 2, me % 2
    twin = chip * 2 + (1 - core)
    partner = (1 - chip) * 2 + core
    low, high = chip == 0, chip == 1
    bf = jnp.bfloat16

    barrier = pltpu.get_barrier_semaphore()
    for other in (twin, partner):
        pl.semaphore_signal(barrier, inc=1, device_id={"sp": other}, device_id_type=pl.DeviceIdType.MESH)

    def remote(src, dst, send, recv, other):
        return pltpu.make_async_remote_copy(src_ref=src, dst_ref=dst, send_sem=send, recv_sem=recv,
                                            device_id={"sp": other}, device_id_type=pl.DeviceIdType.MESH)

    def w_copy(ref, column, slot):
        return pltpu.make_async_copy(ref.at[:, pl.ds(pl.multiple_of(column, TILE), TILE)], w_s.at[slot], w_sem.at[slot])

    def w_proj(kind, s):
        return w_copy((wq_ref, wk_ref, wv_ref)[kind], core * wide + s * TILE, kind)

    def w_wait(slot):
        w_copy(wq_ref, 0, slot).wait()

    rows = own // 4
    mine = core * own

    def x_load(i):
        return pltpu.make_async_copy(x_ref.at[pl.ds(i * rows, rows)], a_s.at[pl.ds(pl.multiple_of(mine + i * rows, rows), rows)], bar_x.at[i])

    for i in range(4):
        x_load(i).start()
    w_proj(0, 0).start()
    w_proj(1, 0).start()
    vt_s[:, HEAD:, :] = jnp.ones_like(vt_s[:, HEAD:, :])
    pl.semaphore_wait(barrier, 2)

    def a_copy(i):
        here = pl.ds(pl.multiple_of(mine + i * rows, rows), rows)
        return remote(a_s.at[here], a_s.at[here], ax_send.at[i], ax_recv.at[i], twin)

    gain = gain_ref[...].astype(jnp.float32)
    for i in range(4):
        x_load(i).wait()

        def norm(j, _):
            here = pl.ds(pl.multiple_of(mine + i * rows + j * 16, 16), 16)
            t = a_s[here, :].astype(jnp.float32)
            scale = lax.rsqrt(jnp.mean(t * t, -1, keepdims=True) + 1e-6)
            a_s[here, :] = (t * scale * gain).astype(bf)

        lax.fori_loop(0, rows // 16, norm, None)
        a_copy(i).start()

    def project(kind, s):
        w_wait(kind)
        for part in range(2):
            base = pl.multiple_of((core if part == 0 else 1 - core) * own, own)
            if kind == 0 and part == 1:
                @pl.when(s == 0)
                def _():
                    for i in range(4):
                        other = pl.ds(pl.multiple_of((1 - core) * own + i * rows, rows), rows)
                        remote(a_s.at[other], a_s.at[other], ax_send.at[i], ax_recv.at[i], twin).wait_recv()
            here = pl.ds(base, own)
            t = _dot(a_s[here, :], w_s[kind]).astype(bf).astype(jnp.float32)
            for j in range(2):
                h = 2 * s + j
                u = t[:, j * HEAD : (j + 1) * HEAD]
                if kind == 0:
                    u = u.T
                    p, q = u[: HEAD // 2], u[HEAD // 2 :]
                    c, d = cos_t[:, here], sin_t[:, here]
                    qt_s[h, : HEAD // 2, here] = (p * c - q * d).astype(bf)
                    qt_s[h, HEAD // 2 :, here] = (q * c + p * d).astype(bf)
                elif kind == 1:
                    k_s[h, here, :] = (u * cos_f[here, :] + pltpu.roll(u, HEAD // 2, 1) * sin_f[here, :]).astype(bf)
                else:
                    vt_s[h, :HEAD, here] = u.T.astype(bf)

    def q_copy(s):
        two = pl.ds(2 * s, 2)
        return remote(qt_s.at[two], xb_s.at[two], q_send.at[s], q_recv.at[s], partner)

    def o_copy(s):
        two = pl.ds(2 * s, 2)
        return remote(xb_s.at[two], xb_s.at[two], o_send.at[s], o_recv.at[s], partner)

    def l_copy(s):
        two = pl.ds(2 * s, 2)
        return remote(lx_s.at[two], lx_s.at[two], l_send.at[s], l_recv.at[s], partner)

    def cross(s):
        def piece(i, _):
            h = 2 * s + i // 2
            firsts = [pl.multiple_of((i % 2) * 2 * STRIP + n * STRIP, STRIP) for n in range(2)]
            scores = [_dot(k_s[h], xb_s[h, :, pl.ds(f, STRIP)]) for f in firsts]
            for n, (f, sc) in enumerate(zip(firsts, scores)):
                top = sc.max(axis=0, keepdims=True)
                weights = jnp.exp2((sc - top) * e).astype(bf)
                mix = _dot(vt_s[h], weights)
                total = mix[HEAD : HEAD + 1]
                xb_s[h, :, pl.ds(f, STRIP)] = (mix[:HEAD] * (1 / total)).astype(bf)
                lx_s[h, :, pl.ds(f, STRIP)] = jnp.broadcast_to(top + jnp.log2(total) * (1 / e), (8, STRIP))

        lax.fori_loop(0, 4, piece, None)

    def step(s, _):
        for kind in range(3):
            @pl.when(s < pairs)
            def _():
                ahead = (kind + 2) % 3
                after = s + (kind + 2) // 3

                @pl.when(after < pairs)
                def _():
                    w_proj(ahead, after).start()

                if kind > 0:
                    @pl.when(after == pairs)
                    def _():
                        w_copy(wo_ref, (kind - 1) * TILE, ahead).start()

                project(kind, s)

            if kind == 0:
                @pl.when(low & (s >= 2))
                def _():
                    o_copy(s - 2).start()
                    l_copy(s - 2).start()

            if kind == 1:
                @pl.when(high & (s < pairs))
                def _():
                    q_copy(s).start()

        @pl.when(low & (s >= 1))
        def _():
            q_copy(s - 1).wait_recv()
            cross(s - 1)

    lax.fori_loop(0, pairs + 1, step, None)

    @pl.when(low)
    def _():
        o_copy(pairs - 1).start()
        l_copy(pairs - 1).start()

    def t_copy(s):
        return remote(o_s.at[2, s], o_s.at[core, s], t_send.at[s], t_recv.at[s], twin)

    keep = lax.broadcasted_iota(jnp.int32, (STRIP, STRIP), 0) <= lax.broadcasted_iota(jnp.int32, (STRIP, STRIP), 1)

    def causal(s, _):
        @pl.when(high)
        def _():
            o_copy(s).wait_recv()
            l_copy(s).wait_recv()

        def head(j):
            h = 2 * s + j
            strips = 2 * own // STRIP
            for i in range(strips):
                at = pl.ds(i * STRIP, STRIP)
                q = qt_s[h, :, at]
                inner = jnp.where(keep, _dot(k_s[h, at, :], q), HIDDEN)
                past = jnp.where(high, lx_s[h, 0:1, at], NEG)
                top = jnp.maximum(inner.max(axis=0, keepdims=True), past)
                if i:
                    outer = _dot(k_s[h, : i * STRIP, :], q)
                    top = jnp.maximum(top, outer.max(axis=0, keepdims=True))
                mix = _dot(vt_s[h, :, at], jnp.exp2((inner - top) * e).astype(bf))
                if i:
                    mix += _dot(vt_s[h, :, : i * STRIP], jnp.exp2((outer - top) * e).astype(bf))
                more = jnp.exp2((past - top) * e)
                total = mix[HEAD : HEAD + 1] + more
                got = (mix[:HEAD] + xb_s[h, :, at].astype(jnp.float32) * more) * (1 / total)
                half = i * STRIP // own
                place = jnp.where(core == half, core, 2)
                o_s[place, s, i * STRIP - half * own : (i + 1) * STRIP - half * own, j * HEAD : (j + 1) * HEAD] = got.T.astype(bf)

        head(0)
        head(1)

        @pl.when(s >= 1)
        def _():
            t_copy(s - 1).start()

    @pl.when(high)
    def _():
        for s in range(pairs):
            q_copy(s).wait_send()

    lax.fori_loop(0, pairs, causal, None)
    t_copy(pairs - 1).start()

    def x_tile(n, slot):
        return pltpu.make_async_copy(x_ref.at[:, pl.ds(pl.multiple_of(n * TILE, TILE), TILE)], xin_s.at[slot], xin_sem.at[slot])

    def y_tile(n, slot):
        return pltpu.make_async_copy(yout_s.at[slot], y_ref.at[:, pl.ds(pl.multiple_of(n * TILE, TILE), TILE)], yout_sem.at[slot])

    x_tile(0, 0).start()
    for s in range(pairs):
        remote(o_s.at[2, s], o_s.at[1 - core, s], t_send.at[s], t_recv.at[s], twin).wait_recv()

    def out(n, _):
        slot, two = n % 3, n % 2

        @pl.when(n + 2 < n_out)
        def _():
            w_copy(wo_ref, (n + 2) * TILE, (n + 2) % 3).start()

        @pl.when(n + 1 < n_out)
        def _():
            x_tile(n + 1, 1 - two).start()

        w_wait(slot)
        seen = jnp.concatenate([o_s[c, s] for c in range(2) for s in range(pairs)], axis=1)
        t = _dot(seen, w_s[slot])
        x_tile(n, two).wait()

        @pl.when(n >= 2)
        def _():
            y_tile(n - 2, two).wait()

        yout_s[two] = (xin_s[two].astype(jnp.float32) + t).astype(bf)
        y_tile(n, two).start()

    lax.fori_loop(0, n_out, out, None)
    y_tile(n_out - 2, 0).wait()
    y_tile(n_out - 1, 1).wait()

    for i in range(4):
        a_copy(i).wait_send()
    for s in range(pairs):
        t_copy(s).wait_send()

    @pl.when(low)
    def _():
        for s in range(pairs):
            o_copy(s).wait_send()
            l_copy(s).wait_send()


def solution(mesh):
    def program(x, gain, wq, wk, wv, wo):
        own, depth = x.shape
        heads = wq.shape[1] // HEAD // 2
        pairs = heads // 2
        chip = lax.axis_index("sp") // 2
        half = HEAD // 2
        place = chip * 2 * own + jnp.arange(2 * own)
        angle = place.astype(jnp.float32)[:, None] * THETA ** (-jnp.arange(half, dtype=jnp.float32) / half)
        cos, sin = jnp.cos(angle), jnp.sin(angle)
        tables = cos.T, sin.T, jnp.concatenate([cos, cos], 1), jnp.concatenate([-sin, sin], 1)
        bf = jnp.bfloat16
        any_, vmem, dma = pl.BlockSpec(memory_space=pl.ANY), pl.BlockSpec(memory_space=pltpu.VMEM), pltpu.SemaphoreType.DMA
        return pl.pallas_call(
            _kernel,
            out_shape=jax.ShapeDtypeStruct(x.shape, bf),
            in_specs=[any_] + [vmem] * 5 + [any_] * 4,
            out_specs=any_,
            scratch_shapes=[
                pltpu.VMEM((2 * own, depth), bf),
                pltpu.VMEM((3, depth, TILE), bf),
                pltpu.VMEM((heads, HEAD, 2 * own), bf),
                pltpu.VMEM((heads, 2 * own, HEAD), bf),
                pltpu.VMEM((heads, HEAD + 16, 2 * own), bf),
                pltpu.VMEM((heads, HEAD, 2 * own), bf),
                pltpu.VMEM((heads, 8, 2 * own), jnp.float32),
                pltpu.VMEM((3, pairs, own, TILE), bf),
                pltpu.VMEM((2, own, TILE), bf),
                pltpu.VMEM((2, own, TILE), bf),
                dma((4,)), dma((3,)), dma((4,)), dma((4,)),
                dma((pairs,)), dma((pairs,)), dma((pairs,)), dma((pairs,)), dma((pairs,)), dma((pairs,)), dma((pairs,)), dma((pairs,)),
                dma((2,)), dma((2,)),
            ],
            compiler_params=pltpu.CompilerParams(collective_id=0, has_side_effects=True, vmem_limit_bytes=67_000_000),
            name="layer",
        )(x, gain.reshape(1, depth), *tables, wq, wk, wv, wo)

    tokens, whole = P(("dp", "sp"), None), P(None, None)
    return jax.shard_map(program, mesh=mesh, in_specs=(tokens, P(None), whole, whole, whole, whole), out_specs=tokens, check_vma=False)
```

```python
import functools

import jax
import jax.numpy as jnp
import numpy as np
from jax import lax
from jax.experimental import pallas as pl
from jax.experimental.pallas import tpu as pltpu
from jax.sharding import PartitionSpec as P

HEAD = 128
THETA = 10000
NEG = -1e30
HIDDEN = 2 * NEG
LOG2E = 1.4426950408889634
TILE = 256
STRIP = 256


def _dot(a, b):
    return jnp.dot(a, b, preferred_element_type=jnp.float32)


def _kernel(x_ref, gain_ref, turn_ref, wq_ref, wk_ref, wv_ref, wo_ref, y_ref,
            a_s, w_s, qt_s, k_s, vt_s, xb_s, lx_s, o_s, s_s, p_s, cos_t, sin_t, cos_f, sin_f, xin_s, yout_s,
            bar_x, w_sem, ax_send, ax_recv, q_send, q_recv, o_send, o_recv, l_send, l_recv, t_send, t_recv, xin_sem, yout_sem, turn_sem):
    own, depth = x_ref.shape
    pairs = k_s.shape[0] // 2
    wide = pairs * TILE
    n_out = depth // TILE
    e = HEAD**-0.5 * LOG2E
    me = lax.axis_index("sp")
    chip, core = me // 2, me % 2
    twin = chip * 2 + (1 - core)
    partner = (1 - chip) * 2 + core
    low, high = chip == 0, chip == 1
    bf = jnp.bfloat16

    barrier = pltpu.get_barrier_semaphore()
    for other in (twin, partner):
        pl.semaphore_signal(barrier, inc=1, device_id={"sp": other}, device_id_type=pl.DeviceIdType.MESH)

    def remote(src, dst, send, recv, other):
        return pltpu.make_async_remote_copy(src_ref=src, dst_ref=dst, send_sem=send, recv_sem=recv,
                                            device_id={"sp": other}, device_id_type=pl.DeviceIdType.MESH)

    def w_copy(ref, column, slot):
        return pltpu.make_async_copy(ref.at[:, pl.ds(pl.multiple_of(column, TILE), TILE)], w_s.at[slot], w_sem.at[slot])

    def w_proj(kind, s):
        return w_copy((wq_ref, wk_ref, wv_ref)[kind], core * wide + s * TILE, kind)

    def w_wait(slot):
        w_copy(wq_ref, 0, slot).wait()

    rows = own // 4
    mine = core * own

    def x_load(i):
        return pltpu.make_async_copy(x_ref.at[pl.ds(i * rows, rows)], a_s.at[pl.ds(pl.multiple_of(mine + i * rows, rows), rows)], bar_x.at[i])

    for i in range(4):
        x_load(i).start()
    turns = [pltpu.make_async_copy(turn_ref.at[i, :, pl.ds(pl.multiple_of(chip * 2 * own, 2 * own), 2 * own)], table, turn_sem.at[i])
             for i, table in enumerate((cos_t, sin_t))]
    for turn in turns:
        turn.start()
    pl.semaphore_wait(barrier, 2)

    def a_copy(i):
        here = pl.ds(pl.multiple_of(mine + i * rows, rows), rows)
        return remote(a_s.at[here], a_s.at[here], ax_send.at[i], ax_recv.at[i], twin)

    gain = gain_ref[...].astype(jnp.float32)[None, :]
    for i in range(4):
        x_load(i).wait()

        def norm(j, _):
            here = pl.ds(pl.multiple_of(mine + i * rows + j * 16, 16), 16)
            t = a_s[here, :].astype(jnp.float32)
            scale = lax.rsqrt(jnp.mean(t * t, -1, keepdims=True) + 1e-6)
            a_s[here, :] = (t * scale * gain).astype(bf)

        lax.fori_loop(0, rows // 16, norm, None)
        a_copy(i).start()
        if i < 3:
            w_proj(i, 0).start()

    def half(kind, s, base):
        here = pl.ds(pl.multiple_of(base, own), own)
        t = _dot(a_s[here, :], w_s[kind]).astype(bf).astype(jnp.float32)
        for j in range(2):
            h = 2 * s + j
            u = t[:, j * HEAD : (j + 1) * HEAD]
            if kind == 0:
                u = u.T
                p, q = u[: HEAD // 2], u[HEAD // 2 :]
                c, d = cos_t[:, here], sin_t[:, here]
                qt_s[h, : HEAD // 2, here] = (p * c - q * d).astype(bf)
                qt_s[h, HEAD // 2 :, here] = (q * c + p * d).astype(bf)
            elif kind == 1:
                k_s[h, here, :] = (u * cos_f[here, :] + pltpu.roll(u, HEAD // 2, 1) * sin_f[here, :]).astype(bf)
            else:
                vt_s[h, :HEAD, here] = u.T.astype(bf)

    def project(kind, s):
        w_wait(kind)
        half(kind, s, 0)
        half(kind, s, own)

    def q_copy(s):
        two = pl.ds(2 * s, 2)
        return remote(qt_s.at[two], xb_s.at[two], q_send.at[s], q_recv.at[s], partner)

    def o_copy(s):
        two = pl.ds(2 * s, 2)
        return remote(xb_s.at[two], xb_s.at[two], o_send.at[s], o_recv.at[s], partner)

    def l_copy(s):
        two = pl.ds(2 * s, 2)
        return remote(lx_s.at[two], lx_s.at[two], l_send.at[s], l_recv.at[s], partner)

    def attention(strips, scores, top_of, finish):
        tops = {}
        for n in range(len(strips) + 2):
            if n >= 2:
                h, at, keys = strips[n - 2]
                finish(h, at, tops[n - 2], _dot(vt_s[h, :, :keys], p_s[n % 2, :keys, :]))
            for first in range(0, 2 * own, STRIP):
                chunk = slice(first, first + STRIP)
                if n < len(strips) and first < strips[n][2]:
                    h, at, keys = strips[n]
                    sc = scores(h, at, keys, chunk)
                    s_s[n % 2, chunk, :] = sc
                    high8 = sc.reshape(STRIP // 8, 8, STRIP).max(axis=0)
                    tops[n] = high8 if first == 0 else jnp.maximum(tops[n], high8)
                if 1 <= n <= len(strips) and first < strips[n - 1][2]:
                    p_s[(n - 1) % 2, chunk, :] = jnp.exp2((s_s[(n - 1) % 2, chunk, :] - tops[n - 1]) * e).astype(bf)
            if n < len(strips):
                tops[n] = top_of(strips[n], tops[n].max(axis=0, keepdims=True))

    def cross(s):
        def scores(h, at, keys, chunk):
            return _dot(k_s[h, chunk, :], xb_s[h, :, at : at + STRIP])

        def finish(h, at, top, mix):
            total = mix[HEAD : HEAD + 1]
            xb_s[h, :, at : at + STRIP] = (mix[:HEAD] * (1 / total)).astype(bf)
            size = top + jnp.log2(total) * (1 / e)
            for i in range(STRIP // HEAD):
                lx_s[h, at // HEAD + i : at // HEAD + i + 1, :] = size[:, i * HEAD : (i + 1) * HEAD]

        attention([(2 * s + j, at, 2 * own) for j in range(2) for at in range(0, 2 * own, STRIP)], scores, lambda strip, top: top, finish)

    def step(s, _):
        for kind in range(3):
            @pl.when(s < pairs)
            def _():
                ahead = (kind + 2) % 3
                after = s + (kind + 2) // 3

                @pl.when(after < pairs)
                def _():
                    w_proj(ahead, after).start()

                if kind > 0:
                    @pl.when(after == pairs)
                    def _():
                        w_copy(wo_ref, (kind - 1) * TILE, ahead).start()

                project(kind, s)

            if kind == 0:
                @pl.when(low & (s >= 2))
                def _():
                    o_copy(s - 2).start()
                    l_copy(s - 2).start()

            if kind == 1:
                @pl.when(high & (s < pairs))
                def _():
                    q_copy(s).start()

        @pl.when(low)
        def _():
            q_copy(s - 1).wait_recv()
            cross(s - 1)

    for turn in turns:
        turn.wait()
    for kind in range(3):
        w_wait(kind)
        if kind == 0:
            vt_s[:, HEAD:, :] = jnp.ones_like(vt_s[:, HEAD:, :])
            c, d = cos_t[...].T, sin_t[...].T
            cos_f[...] = jnp.concatenate([c, c], axis=1)
            sin_f[...] = jnp.concatenate([-d, d], axis=1)
        half(kind, 0, core * own)
    for i in range(4):
        other = pl.ds(pl.multiple_of((1 - core) * own + i * rows, rows), rows)
        remote(a_s.at[other], a_s.at[other], ax_send.at[i], ax_recv.at[i], twin).wait_recv()
    for kind in range(3):
        half(kind, 0, (1 - core) * own)
        if kind < 2:
            w_proj(kind, 1).start()
        if kind == 1:
            @pl.when(high)
            def _():
                q_copy(0).start()

    lax.fori_loop(1, pairs + 1, step, None)

    @pl.when(low)
    def _():
        o_copy(pairs - 1).start()
        l_copy(pairs - 1).start()

    def t_copy(s):
        return remote(o_s.at[2, s], o_s.at[core, s], t_send.at[s], t_recv.at[s], twin)

    keep = lax.broadcasted_iota(jnp.int32, (STRIP, STRIP), 0) <= lax.broadcasted_iota(jnp.int32, (STRIP, STRIP), 1)

    def causal(s, _):
        @pl.when(high)
        def _():
            o_copy(s).wait_recv()
            l_copy(s).wait_recv()

        def scores(h, at, keys, chunk):
            sc = _dot(k_s[h, chunk, :], qt_s[h, :, at : at + STRIP])
            return jnp.where(keep, sc, HIDDEN) if chunk.stop == keys else sc

        def past(h, at):
            size = [lx_s[h, at // HEAD + i : at // HEAD + i + 1, :] for i in range(STRIP // HEAD)]
            return jnp.where(high, jnp.concatenate(size, axis=1), NEG)

        def finish(h, at, top, mix):
            more = jnp.exp2((past(h, at) - top) * e)
            total = mix[HEAD : HEAD + 1] + more
            got = (mix[:HEAD] + xb_s[h, :, at : at + STRIP].astype(jnp.float32) * more) * (1 / total)
            place = jnp.where(core == at // own, core, 2)
            j = js[0]
            js[0] = 1 - j if (at + STRIP == 2 * own) else j
            o_s[place, s, at % own : at % own + STRIP, j * HEAD : (j + 1) * HEAD] = got.T.astype(bf)

        js = [0]
        attention([(2 * s + j, at, at + STRIP) for j in range(2) for at in range(0, 2 * own, STRIP)], scores,
                  lambda strip, top: jnp.maximum(top, past(*strip[:2])), finish)

        @pl.when(s >= 1)
        def _():
            t_copy(s - 1).start()

    lax.fori_loop(0, pairs, causal, None)
    t_copy(pairs - 1).start()

    def x_tile(n, slot):
        return pltpu.make_async_copy(x_ref.at[:, pl.ds(pl.multiple_of(n * TILE, TILE), TILE)], xin_s.at[slot], xin_sem.at[slot])

    def y_tile(n, slot):
        return pltpu.make_async_copy(yout_s.at[slot], y_ref.at[:, pl.ds(pl.multiple_of(n * TILE, TILE), TILE)], yout_sem.at[slot])

    x_tile(0, 0).start()
    for s in range(pairs):
        remote(o_s.at[2, s], o_s.at[1 - core, s], t_send.at[s], t_recv.at[s], twin).wait_recv()

    def out(n, _):
        slot, two = n % 3, n % 2

        @pl.when(n + 2 < n_out)
        def _():
            w_copy(wo_ref, (n + 2) * TILE, (n + 2) % 3).start()

        @pl.when(n + 1 < n_out)
        def _():
            x_tile(n + 1, 1 - two).start()

        w_wait(slot)
        seen = jnp.concatenate([o_s[c, s] for c in range(2) for s in range(pairs)], axis=1)
        t = _dot(seen, w_s[slot])
        x_tile(n, two).wait()

        @pl.when(n >= 2)
        def _():
            y_tile(n - 2, two).wait()

        yout_s[two] = (xin_s[two].astype(jnp.float32) + t).astype(bf)
        y_tile(n, two).start()

    lax.fori_loop(0, n_out, out, None)
    y_tile(n_out - 2, 0).wait()
    y_tile(n_out - 1, 1).wait()

    for i in range(4):
        a_copy(i).wait_send()
    for s in range(pairs):
        t_copy(s).wait_send()

    @pl.when(high)
    def _():
        for s in range(pairs):
            q_copy(s).wait_send()

    @pl.when(low)
    def _():
        for s in range(pairs):
            o_copy(s).wait_send()
            l_copy(s).wait_send()


def turns(tokens):
    half = HEAD // 2
    rate = (np.float32(THETA) ** (-np.arange(half, dtype=np.float32) / np.float32(half))).astype(np.float32)
    angle = np.arange(tokens, dtype=np.float32)[None, :] * rate[:, None]
    wide = angle.astype(np.float64)
    return np.stack([np.cos(wide), np.sin(wide)]).astype(np.float32)


def solution(mesh):
    def program(x, gain, wq, wk, wv, wo):
        own, depth = x.shape
        heads = wq.shape[1] // HEAD // 2
        pairs = heads // 2
        bf = jnp.bfloat16
        turn = jnp.asarray(turns(own * mesh.shape["sp"]))
        any_, vmem, dma = pl.BlockSpec(memory_space=pl.ANY), pl.BlockSpec(memory_space=pltpu.VMEM), pltpu.SemaphoreType.DMA
        return pl.pallas_call(
            _kernel,
            out_shape=jax.ShapeDtypeStruct(x.shape, bf),
            in_specs=[any_, vmem] + [any_] * 5,
            out_specs=any_,
            scratch_shapes=[
                pltpu.VMEM((2 * own, depth), bf),
                pltpu.VMEM((3, depth, TILE), bf),
                pltpu.VMEM((heads, HEAD, 2 * own), bf),
                pltpu.VMEM((heads, 2 * own, HEAD), bf),
                pltpu.VMEM((heads, HEAD + 16, 2 * own), bf),
                pltpu.VMEM((heads, HEAD, 2 * own), bf),
                pltpu.VMEM((heads, 2 * own // HEAD, HEAD), jnp.float32),
                pltpu.VMEM((3, pairs, own, TILE), bf),
                pltpu.VMEM((2, 2 * own, STRIP), jnp.float32),
                pltpu.VMEM((2, 2 * own, STRIP), bf),
                pltpu.VMEM((HEAD // 2, 2 * own), jnp.float32),
                pltpu.VMEM((HEAD // 2, 2 * own), jnp.float32),
                pltpu.VMEM((2 * own, HEAD), jnp.float32),
                pltpu.VMEM((2 * own, HEAD), jnp.float32),
                pltpu.VMEM((2, own, TILE), bf),
                pltpu.VMEM((2, own, TILE), bf),
                dma((4,)), dma((3,)), dma((4,)), dma((4,)),
                dma((pairs,)), dma((pairs,)), dma((pairs,)), dma((pairs,)), dma((pairs,)), dma((pairs,)), dma((pairs,)), dma((pairs,)),
                dma((2,)), dma((2,)), dma((2,)),
            ],
            compiler_params=pltpu.CompilerParams(collective_id=0, has_side_effects=True, vmem_limit_bytes=67_000_000),
            name="layer",
        )(x, gain, turn, wq, wk, wv, wo)

    tokens, whole = P(("dp", "sp"), None), P(None, None)
    return jax.shard_map(program, mesh=mesh, in_specs=(tokens, P(None), whole, whole, whole, whole), out_specs=tokens, check_vma=False)
```

```python
import functools

import jax
import jax.numpy as jnp
import numpy as np
from jax import lax
from jax.experimental import pallas as pl
from jax.experimental.pallas import tpu as pltpu
from jax.sharding import PartitionSpec as P

HEAD = 128
THETA = 10000
NEG = -1e30
HIDDEN = 2 * NEG
LOG2E = 1.4426950408889634
TILE = 256
STRIP = 256
EARLY = 7
TWICE = 14
MOVED = 2


def _dot(a, b):
    return jnp.dot(a, b, preferred_element_type=jnp.float32)


def _kernel(x_ref, gain_ref, turn_ref, wq_ref, wk_ref, wv_ref, wo_ref, y_ref,
            a_s, w_s, qt_s, k_s, vt_s, xb_s, lx_s, o_s, s_s, p_s, top_s, last_s, t_s, cos_t, sin_t, cs_f, acc_s, io_s,
            bar_x, w_sem, ax_send, ax_recv, q_send, q_recv, o_send, o_recv, l_send, l_recv, tw_send, tw_recv, kv_send, kv_recv, wo_sem, io_sem, turn_sem):
    own, depth = x_ref.shape
    pairs = (o_s.shape[0] - 2) // 2
    moved = k_s.shape[0] // 2 - pairs
    wide = pairs * TILE
    few = wide - EARLY * TILE
    n_out = depth // TILE
    e = HEAD**-0.5 * LOG2E
    me = lax.axis_index("sp")
    chip, core = me // 2, me % 2
    twin = chip * 2 + (1 - core)
    partner = (1 - chip) * 2 + core
    low, high = chip == 0, chip == 1
    bf = jnp.bfloat16

    barrier = pltpu.get_barrier_semaphore()
    for other in (twin, partner):
        pl.semaphore_signal(barrier, inc=1, device_id={"sp": other}, device_id_type=pl.DeviceIdType.MESH)

    def remote(src, dst, send, recv, other):
        return pltpu.make_async_remote_copy(src_ref=src, dst_ref=dst, send_sem=send, recv_sem=recv,
                                            device_id={"sp": other}, device_id_type=pl.DeviceIdType.MESH)

    def pair_of(s):
        return jnp.where(low, s, (s + moved) % pairs)

    def w_copy(ref, column, slot):
        return pltpu.make_async_copy(ref.at[:, pl.ds(pl.multiple_of(column, TILE), TILE)], w_s.at[slot], w_sem.at[slot])

    def w_proj(kind, s):
        return w_copy((wq_ref, wk_ref, wv_ref)[kind], core * wide + pair_of(s) * TILE, kind)

    def wo_rows(n, soon):
        copies = []
        for g in range(2):
            many = EARLY * TILE if soon else few
            here = pl.ds(g * wide + (0 if soon else EARLY * TILE), many)
            there = pl.ds(pl.multiple_of((g if soon else 2 * (n // 3 % 3) + g) * many, many), many)
            column = pl.ds(pl.multiple_of(n * TILE, TILE), TILE)
            copies += [pltpu.make_async_copy(wo_ref.at[here, column], w_s.at[n % 3, there], wo_sem.at[n % 9, g])]
        return copies

    def w_wait(slot):
        w_copy(wq_ref, 0, slot).wait()

    rows = own // 4
    mine = core * own

    def x_load(i):
        return pltpu.make_async_copy(x_ref.at[pl.ds(i * rows, rows)], a_s.at[pl.ds(pl.multiple_of(mine + i * rows, rows), rows)], bar_x.at[i])

    for i in range(4):
        x_load(i).start()
    turns = [pltpu.make_async_copy(turn_ref.at[i], table, turn_sem.at[i]) for i, table in enumerate((cos_t, sin_t))]
    for turn in turns:
        turn.start()
    pl.semaphore_wait(barrier, 2)

    def a_copy(i):
        here = pl.ds(pl.multiple_of(mine + i * rows, rows), rows)
        return remote(a_s.at[here], a_s.at[here], ax_send.at[i], ax_recv.at[i], twin)

    gain = gain_ref[...].astype(jnp.float32)[None, :]
    for i in range(4):
        x_load(i).wait()

        def norm(j, _):
            here = pl.ds(pl.multiple_of(mine + i * rows + j * 16, 16), 16)
            t = a_s[here, :].astype(jnp.float32)
            scale = lax.rsqrt(jnp.mean(t * t, -1, keepdims=True) + 1e-6)
            a_s[here, :] = (t * scale * gain).astype(bf)

        lax.fori_loop(0, rows // 16, norm, None)
        a_copy(i).start()
        if i < 3:
            w_proj(i, 0).start()

    def product(kind, base, size=own):
        here = pl.ds(pl.multiple_of(base, size), size)
        t_s[kind, here, :] = _dot(a_s[here, :], w_s[kind]).astype(bf)

    def epilogue(kind, pair, base):
        here = pl.ds(pl.multiple_of(base, own), own)
        if kind == 1:
            both = cs_f[here, :]
            other = pltpu.roll(both, HEAD // 2, 1)
            first = lax.broadcasted_iota(jnp.int32, both.shape, 1) < HEAD // 2
            cos, sin = jnp.where(first, both, other), jnp.where(first, -other, both)
        for j in range(2):
            h = 2 * pair + j
            u = t_s[kind, here, j * HEAD : (j + 1) * HEAD].astype(jnp.float32)
            if kind == 0:
                u = u.T
                p, q = u[: HEAD // 2], u[HEAD // 2 :]
                c, d = cos_t[:, here], sin_t[:, here]
                qt_s[h, : HEAD // 2, here] = (p * c - q * d).astype(bf)
                qt_s[h, HEAD // 2 :, here] = (q * c + p * d).astype(bf)
            elif kind == 1:
                k_s[h, here, :] = (u * cos + pltpu.roll(u, HEAD // 2, 1) * sin).astype(bf)
            else:
                vt_s[h, :HEAD, here] = u.T.astype(bf)

    def before(kind, s):
        return (kind + 2) % 3, pair_of(s - 1 if kind == 0 else s)

    def tile(kind, s):
        w_wait(kind)

        def part(i, _):
            epilogue(*before(kind, s), i * own)
            product(kind, i * own)

        lax.fori_loop(0, 2, part, None)

    def q_copy(s):
        two = pl.ds(2 * s, 2)
        return remote(qt_s.at[two], xb_s.at[two], q_send.at[s], q_recv.at[s], partner)

    def o_copy(s):
        two = pl.ds(2 * s, 2)
        return remote(xb_s.at[two], xb_s.at[two], o_send.at[s], o_recv.at[s], partner)

    def l_copy(s):
        two = pl.ds(2 * s, 2)
        return remote(lx_s.at[two], lx_s.at[two], l_send.at[s], l_recv.at[s], partner)

    def pair_at(n):
        return jnp.where(low, (n + moved) % pairs, n)

    def staged(pair):
        return 2 * pairs + jnp.where(low, pair + pairs - moved, pair) % pairs % 2

    def t_copy(s):
        return remote(o_s.at[staged(s)], o_s.at[core * pairs + s], tw_send.at[s], tw_recv.at[s], twin)

    def kv_copies(i):
        src, dst = pl.ds(2 * i, 2), pl.ds(2 * (pairs + i), 2)
        return [remote(k_s.at[src], k_s.at[dst], kv_send.at[i, 0], kv_recv.at[i, 0], partner),
                remote(vt_s.at[src, :HEAD], vt_s.at[dst, :HEAD], kv_send.at[i, 1], kv_recv.at[i, 1], partner)]

    def make_scores(strips, scores, top_of, slot):
        place = 0
        for i, strip in enumerate(strips):
            top = None
            for first in range(0, strip[2], STRIP):
                sc = scores(*strip, slice(first, first + STRIP))
                s_s[slot, place + first : place + first + STRIP, :] = sc
                high8 = sc.reshape(STRIP // 8, 8, STRIP).max(axis=0)
                top = high8 if top is None else jnp.maximum(top, high8)
            place += strip[2]
            top_s[slot, i : i + 1, :] = top_of(strip, top.max(axis=0, keepdims=True))

    def make_weights(strips, slot):
        place = 0
        for i, strip in enumerate(strips):
            top = top_s[slot, i : i + 1, :]
            for first in range(place, place + strip[2], STRIP):
                p_s[slot, first : first + STRIP, :] = jnp.exp2((s_s[slot, first : first + STRIP, :] - top) * e).astype(bf)
            place += strip[2]

    def make_mix(strips, finish, slot):
        place = 0
        for i, strip in enumerate(strips):
            h, at, keys, g = strip
            finish(h, at, last_s[slot, i : i + 1, :], _dot(vt_s[g, :, :keys], p_s[slot, place : place + keys, :]))
            place += keys

    def keep_tops(strips, slot):
        for i in range(len(strips)):
            last_s[slot, i : i + 1, :] = top_s[slot, i : i + 1, :]

    def attention(jobs):
        for n in range(len(jobs) + 2):
            stage(jobs, n)

    def stage(jobs, n):
        if 2 <= n < len(jobs) + 2:
            make_mix(jobs[n - 2][0], jobs[n - 2][3], n % 2)
        if 1 <= n < len(jobs) + 1:
            make_weights(jobs[n - 1][0], (n - 1) % 2)
            keep_tops(jobs[n - 1][0], (n - 1) % 2)
        if n < len(jobs):
            make_scores(*jobs[n][:3], n % 2)

    def cross_jobs(pair, first):
        def scores(h, at, keys, g, chunk):
            return _dot(k_s[g, chunk, :], xb_s[h, :, at : at + STRIP])

        def finish(h, at, top, mix):
            total = mix[HEAD : HEAD + 1]
            xb_s[h, :, at : at + STRIP] = (mix[:HEAD] * (1 / total)).astype(bf)
            size = top + jnp.log2(total) * (1 / e)
            for i in range(STRIP // HEAD):
                lx_s[h, at // HEAD + i : at // HEAD + i + 1, :] = size[:, i * HEAD : (i + 1) * HEAD]

        strips = [(2 * pair + j, at, 2 * own, first + j) for j in range(2) for at in range(0, 2 * own, STRIP)]
        return [([strip], scores, lambda strip, top: top, finish) for strip in strips]

    keep = lax.broadcasted_iota(jnp.int32, (STRIP, STRIP), 0) <= lax.broadcasted_iota(jnp.int32, (STRIP, STRIP), 1)

    def causal_jobs(pair, taking):
        def scores(h, at, keys, g, chunk):
            sc = _dot(k_s[g, chunk, :], qt_s[h, :, at : at + STRIP])
            return jnp.where(keep, sc, HIDDEN) if chunk.stop == keys else sc

        def past(h, at):
            size = [lx_s[h, at // HEAD + i : at // HEAD + i + 1, :] for i in range(STRIP // HEAD)]
            return jnp.where(high, jnp.concatenate(size, axis=1), NEG)

        def finish(h, at, top, mix, j):
            total, got = mix[HEAD : HEAD + 1], mix[:HEAD]
            if taking:
                more = jnp.exp2((past(h, at) - top) * e)
                total = total + more
                got = got + jnp.where(high, xb_s[h, :, at : at + STRIP].astype(jnp.float32), 0.0) * more
            place = jnp.where(core == at // own, core * pairs + pair, staged(pair))
            o_s[place, at % own : at % own + STRIP, j * HEAD : (j + 1) * HEAD] = (got * (1 / total)).T.astype(bf)

        def top_of(strip, top):
            return jnp.maximum(top, past(*strip[:2])) if taking else top

        jobs = []
        for j in range(2):
            h = 2 * pair + j
            for i in range(own // STRIP):
                strips = [(h, at, at + STRIP, h) for at in (i * STRIP, 2 * own - (i + 1) * STRIP)]
                jobs += [(strips, scores, top_of, functools.partial(finish, j=j))]
        return jobs

    def step(s, _):
        c = s - 1
        for kind in range(3):
            ahead = (kind + 2) % 3
            after = s + (kind + 2) // 3

            @pl.when(after < pairs)
            def _():
                w_proj(ahead, after).start()

            if kind > 0:
                @pl.when(low & (after == pairs))
                def _():
                    w_copy(wo_ref, (kind - 1) * TILE, ahead).start()

                @pl.when(high & (after == pairs))
                def _():
                    for copy in wo_rows(kind - 1, True):
                        copy.start()

            @pl.when(high | (c < moved))
            def _():
                tile(kind, s)

            for i in range(4):
                @pl.when(low & (c >= moved))
                def _():
                    n = 4 * kind + i
                    jobs = cross_jobs(c, 2 * c) + causal_jobs(c, False)
                    if i == 0:
                        w_wait(kind)
                        if kind == 0:
                            @pl.when(c >= moved + 2)
                            def _():
                                t_copy(c - 2).wait_send()

                            q_copy(c).wait_recv()
                            stage(jobs, 0)
                        for first in range(0, 2 * own, own):
                            epilogue(*before(kind, s), first)
                    product(kind, i * STRIP, STRIP)
                    stage(jobs, n + 1)

            if kind == 2:
                @pl.when(low & (c >= moved))
                def _():
                    stage(cross_jobs(c, 2 * c) + causal_jobs(c, False), 13)

            if kind == 0:
                @pl.when(low & (c >= moved + 1))
                def _():
                    t_copy(c - 1).start()

            if kind == 0 and moved:
                @pl.when(low & (s - 1 < moved))
                def _():
                    kv_copies(s - 1)[1].start()

            if kind == 2 and moved > 1:
                @pl.when(low & (s < moved))
                def _():
                    kv_copies(s)[0].start()

            if kind == 2:
                @pl.when(low & (c >= moved))
                def _():
                    o_copy(c).start()
                    l_copy(c).start()

                @pl.when(high & (s < pairs - moved))
                def _():
                    q_copy(s + moved).start()

    for turn in turns:
        turn.wait()
    vt_s[:, HEAD:, :] = jnp.ones_like(vt_s[:, HEAD:, :])
    c, d = cos_t[:, : 2 * own], sin_t[:, : 2 * own]
    p, q = jnp.where(low, 1.0, cos_t[:, 2 * own : 2 * own + 1]), jnp.where(low, 0.0, sin_t[:, 2 * own : 2 * own + 1])
    c, d = c * p - d * q, d * p + c * q
    cos_t[:, : 2 * own] = c
    sin_t[:, : 2 * own] = d
    c, d = c.T, d.T
    cs_f[...] = jnp.concatenate([c, d], axis=1)
    for kind in range(3):
        w_wait(kind)

    def early(kind, _):
        product(kind, core * own)

    def late(kind, _):
        product(kind, (1 - core) * own)

    lax.fori_loop(0, 3, early, None)
    for i in range(4):
        other = pl.ds(pl.multiple_of((1 - core) * own + i * rows, rows), rows)
        remote(a_s.at[other], a_s.at[other], ax_send.at[i], ax_recv.at[i], twin).wait_recv()
    lax.fori_loop(0, 3, late, None)
    w_proj(0, 1).start()
    w_proj(1, 1).start()
    for kind in range(2):
        for first in range(0, 2 * own, own):
            epilogue(kind, pair_of(0), first)

    if moved:
        @pl.when(low)
        def _():
            kv_copies(0)[0].start()

    @pl.when(high)
    def _():
        q_copy(moved).start()

    lax.fori_loop(1, pairs, step, None)
    for first in range(0, 2 * own, own):
        epilogue(2, pair_of(pairs - 1), first)
    final = pairs - 1

    @pl.when(low)
    def _():
        t_copy(final - 1).start()
        q_copy(final).wait_recv()

    @pl.when(high)
    def _():
        for i in range(moved):
            for copy in kv_copies(i):
                copy.wait_recv()
        if moved:
            xb_s[: 2 * moved] = qt_s[: 2 * moved]

    def rest(i, _):
        pair = jnp.where(low, final, i)
        attention(cross_jobs(pair, jnp.where(low, 2 * pair, 2 * (pairs + i))))

    lax.fori_loop(0, jnp.where(low, 1, moved), rest, None)

    @pl.when(low)
    def _():
        o_copy(final).start()
        l_copy(final).start()

    skipped = jnp.where(low, pairs - 1 - moved, 0)

    def t_arrived(s):
        remote(o_s.at[staged(s)], o_s.at[(1 - core) * pairs + s], tw_send.at[s], tw_recv.at[s], twin).wait_recv()

    def mixed(n, first, last):
        rows = 2 * (last - first) * TILE
        at = 0 if first == 0 else pl.multiple_of(n // 3 % 3 * rows, rows)
        seen = jnp.concatenate([o_s[g * pairs + s] for g in range(2) for s in range(first, last)], axis=1)
        return _dot(seen, w_s[n % 3, pl.ds(at, rows), :])

    def x_tile(n, slot):
        return pltpu.make_async_copy(x_ref.at[:, pl.ds(pl.multiple_of(n * TILE, TILE), TILE)], io_s.at[slot], io_sem.at[slot])

    def y_tile(n, slot):
        return pltpu.make_async_copy(io_s.at[slot], y_ref.at[:, pl.ds(pl.multiple_of(n * TILE, TILE), TILE)], io_sem.at[slot])

    def soon(n, _):
        @pl.when(n + 2 < TWICE)
        def _():
            for copy in wo_rows(n + 2, True):
                copy.start()

        @pl.when(n + 1 < TWICE)
        def _():
            x_tile(n + 1, (n + 1) % 2).start()

        for copy in wo_rows(n, True):
            copy.wait()
        x_tile(n, n % 2).wait()
        acc_s[n] = io_s[n % 2].astype(jnp.float32) + mixed(n, 0, EARLY)

    def late(i, _):
        slots = [2 * (i % 2) + k for k in range(2)]
        for k in range(2):
            n = 2 * i + k

            @pl.when(i >= 2)
            def _():
                y_tile(n - 4, slots[k]).wait()

            @pl.when(n + 6 < TWICE)
            def _():
                for copy in wo_rows(n + 6, False):
                    copy.start()

        @pl.when(i == TWICE // 2 - 1)
        def _():
            w_copy(wo_ref, TWICE * TILE, TWICE % 3).start()

        for k in range(2):
            for copy in wo_rows(2 * i + k, False):
                copy.wait()
        for k in range(2):
            io_s[slots[k]] = (acc_s[2 * i + k] + mixed(2 * i + k, EARLY, pairs)).astype(bf)
        for k in range(2):
            y_tile(2 * i + k, slots[k]).start()

    def within(i, _):
        pair = pair_at(i)

        @pl.when(i > skipped)
        def _():
            t_copy(pair_at(i - 1)).start()

        @pl.when(i >= 2)
        def _():
            t_copy(pair_at(i - 2)).wait_send()

        @pl.when(high & (i == EARLY))
        def _():
            for s in range(EARLY):
                t_arrived(s)
            x_tile(0, 0).start()
            lax.fori_loop(0, TWICE, soon, None)
            for n in range(6):
                for copy in wo_rows(n, False):
                    copy.start()

        @pl.when(high & (pair >= moved))
        def _():
            o_copy(pair).wait_recv()
            l_copy(pair).wait_recv()

        attention(causal_jobs(pair, True))

    lax.fori_loop(skipped, pairs, within, None)
    t_copy(pair_at(pairs - 1)).start()

    @pl.when(low)
    def _():
        x_tile(0, 0).start()
        for s in range(EARLY):
            t_arrived(s)

    for s in range(EARLY, pairs):
        t_arrived(s)

    @pl.when(high)
    def _():
        lax.fori_loop(0, TWICE // 2, late, None)
        w_copy(wo_ref, (TWICE + 1) * TILE, (TWICE + 1) % 3).start()
        for n in range(TWICE - 4, TWICE):
            y_tile(n, n % 2 + 2 * (n // 2 % 2)).wait()
        x_tile(TWICE, 0).start()

    begin = jnp.where(low, 0, TWICE)

    def out(n, _):
        two = n % 2

        @pl.when(n + 2 < n_out)
        def _():
            w_copy(wo_ref, (n + 2) * TILE, (n + 2) % 3).start()

        @pl.when(n + 1 < n_out)
        def _():
            x_tile(n + 1, 1 - two).start()

        x_tile(n, two).wait()

        @pl.when(n >= begin + 2)
        def _():
            y_tile(n - 2, 2 + two).wait()

        w_wait(n % 3)
        seen = jnp.concatenate([o_s[s] for s in range(2 * pairs)], axis=1)
        io_s[2 + two] = (io_s[two].astype(jnp.float32) + _dot(seen, w_s[n % 3])).astype(bf)
        y_tile(n, 2 + two).start()

    lax.fori_loop(begin, n_out, out, None)
    y_tile(n_out - 2, 2).wait()
    y_tile(n_out - 1, 3).wait()

    for i in range(4):
        a_copy(i).wait_send()
    for n in range(pairs - 2, pairs):
        t_copy(pair_at(n)).wait_send()

    @pl.when(high)
    def _():
        for s in range(moved, pairs):
            q_copy(s).wait_send()

    @pl.when(low)
    def _():
        for s in range(moved, pairs):
            o_copy(s).wait_send()
            l_copy(s).wait_send()
        for i in range(moved):
            for copy in kv_copies(i):
                copy.wait_send()


def turns(tokens):
    half = HEAD // 2
    rate = (np.float32(THETA) ** (-np.arange(half, dtype=np.float32) / np.float32(half))).astype(np.float32)
    place = np.concatenate([np.arange(tokens), np.full(HEAD, tokens)]).astype(np.float32)
    angle = place[None, :] * rate[:, None]
    wide = angle.astype(np.float64)
    return np.stack([np.cos(wide), np.sin(wide)]).astype(np.float32)


def solution(mesh):
    def program(x, gain, wq, wk, wv, wo):
        own, depth = x.shape
        heads = wq.shape[1] // HEAD // 2
        pairs = heads // 2
        bf = jnp.bfloat16
        turn = jnp.asarray(turns(2 * own))
        any_, vmem, dma = pl.BlockSpec(memory_space=pl.ANY), pl.BlockSpec(memory_space=pltpu.VMEM), pltpu.SemaphoreType.DMA
        return pl.pallas_call(
            _kernel,
            out_shape=jax.ShapeDtypeStruct(x.shape, bf),
            in_specs=[any_, vmem] + [any_] * 5,
            out_specs=any_,
            scratch_shapes=[
                pltpu.VMEM((2 * own, depth), bf),
                pltpu.VMEM((3, depth, TILE), bf),
                pltpu.VMEM((heads, HEAD, 2 * own), bf),
                pltpu.VMEM((heads + 2 * MOVED, 2 * own, HEAD), bf),
                pltpu.VMEM((heads + 2 * MOVED, HEAD + 16, 2 * own), bf),
                pltpu.VMEM((heads, HEAD, 2 * own), bf),
                pltpu.VMEM((heads, 2 * own // HEAD, HEAD), jnp.float32),
                pltpu.VMEM((2 * pairs + 2, own, TILE), bf),
                pltpu.VMEM((2, 2 * own + STRIP, STRIP), jnp.float32),
                pltpu.VMEM((2, 2 * own + STRIP, STRIP), bf),
                pltpu.VMEM((2, 8, STRIP), jnp.float32),
                pltpu.VMEM((2, 8, STRIP), jnp.float32),
                pltpu.VMEM((3, 2 * own, TILE), bf),
                pltpu.VMEM((HEAD // 2, 2 * own + HEAD), jnp.float32),
                pltpu.VMEM((HEAD // 2, 2 * own + HEAD), jnp.float32),
                pltpu.VMEM((2 * own, HEAD), jnp.float32),
                pltpu.VMEM((TWICE, own, TILE), jnp.float32),
                pltpu.VMEM((4, own, TILE), bf),
                dma((4,)), dma((3,)), dma((4,)), dma((4,)),
                dma((pairs,)), dma((pairs,)), dma((pairs,)), dma((pairs,)), dma((pairs,)), dma((pairs,)), dma((pairs,)), dma((pairs,)),
                dma((max(MOVED, 1), 2)), dma((max(MOVED, 1), 2)),
                dma((9, 2)), dma((4,)), dma((2,)),
            ],
            compiler_params=pltpu.CompilerParams(collective_id=0, has_side_effects=True, vmem_limit_bytes=67_000_000),
            name="layer",
        )(x, gain, turn, wq, wk, wv, wo)

    tokens, whole = P(("dp", "sp"), None), P(None, None)
    return jax.shard_map(program, mesh=mesh, in_specs=(tokens, P(None), whole, whole, whole, whole), out_specs=tokens, check_vma=False)
```
